32 devices in a mesh: rows: 16 (over z, y, x), rhs: 2 (over core).
Axes of the slice: x: 2, y: 2, z: 4, core: 2. Of those that a mesh axis runs over, the one named last changes fastest.
Arguments:
- rhs: float32 [2, 8192, 4096], P(None, 'rows', 'rhs'), may hold values from -8 to 8
- factor: bfloat16 [2, 8192, 4, 512], P(None, 'rows', None, 'rhs'), may hold values from -0.125 to 0.125
- inverses: float32 [4, 512, 512], replicated, may hold values from -1 to 1, as said below
Outputs:
- state: float32 [2, 8192, 4096], P(None, 'rows', 'rhs')
The draws below stay inside these ranges and needn't reach their ends.
Inputs may be any that keep to these rules, and one draw needn't show every extreme that they name: Each inverses[p] is unit lower triangular: ones on the diagonal, zeros above it.
All inputs are finite; a program needn't handle non-finite values.
Results may differ from the reference program's by a relative error of at most 0.003.
Values may be sent and summed in bfloat16 or wider, within the bound.
A program may use at most 128 MiB of HBM per device.

```python
import jax
import jax.numpy as jnp
from jax import lax

TILE = 512
PANELS = 4
NRHS = 4096
CYC = 2
WIDTH = 8192
N_ROWS = 16


def draw_inverses(key, part):
    values = jax.random.normal(key, (PANELS, TILE, TILE), jnp.float32)
    values = jnp.clip(values, -4.0, 4.0) * TILE ** (-0.5)
    return jnp.tril(values, -1) + jnp.eye(TILE, dtype=jnp.float32)[None]


def level_of(rng, shape, cuts, low, high):
    loudness, own = 1.0, jax.random.fold_in(rng, 6)
    for axis_at, shards_of in cuts:
        steps = jnp.exp(jax.random.uniform(jax.random.fold_in(own, axis_at), (shards_of,), jnp.float32, low / len(cuts), high / len(cuts)))
        loudness = loudness * jnp.repeat(steps, shape[axis_at] // shards_of).reshape([-1 if axis == axis_at else 1 for axis in range(len(shape))])
    return loudness


def bell_draw(key, dims, scale, reach, split=(), kind=jnp.bfloat16):
    result = jax.random.normal(key, dims, jnp.float32) * scale
    if len(split) > 0:
        result = level_of(key, dims, split, -0.22, 0.18) * result
    return jnp.clip(result, min=-reach, max=reach).astype(kind)


def setup_inputs(seed: int = 0) -> dict:
    keys = jax.random.split(jax.random.key(seed), 4)
    rhs = bell_draw(keys[0], (CYC, WIDTH, NRHS), 1.0, 8.0, ((1, 16), (2, 2)), jnp.float32)
    factor = bell_draw(keys[1], (CYC, WIDTH, PANELS, TILE), (PANELS * TILE) ** -0.5, 0.125, ((1, 16), (3, 2)))
    inverses = draw_inverses(jax.random.fold_in(keys[3], 71), 0)
    return {"rhs": rhs, "factor": factor, "inverses": inverses}


def reference(rhs, factor, inverses):
    cycles = rhs.shape[0]
    width = rhs.shape[1]
    tile_ids = jnp.arange(cycles, dtype=jnp.int32)[:, None] * N_ROWS + (jnp.arange(width, dtype=jnp.int32) // TILE)[None, :]
    state = rhs
    for panel in range(PANELS):
        pivot = state[0, panel * TILE:(panel + 1) * TILE]
        solved = jnp.dot(inverses[panel], pivot, precision=lax.Precision.HIGHEST)
        sent = lax.optimization_barrier(solved.astype(jnp.bfloat16)).astype(jnp.float32)
        state = state.at[0, panel * TILE:(panel + 1) * TILE].set(solved)
        delta = jnp.einsum("crk,kn->crn", factor[:, :, panel, :].astype(jnp.float32), sent, precision=lax.Precision.HIGHEST)
        state = state - jnp.where((tile_ids > panel)[:, :, None], delta, jnp.float32(0.0))
    return state
```

```python
import jax
import jax.numpy as jnp
from jax import lax
from jax.sharding import PartitionSpec as P


def local(rhs, factor, inverses):
    count = lax.axis_size("rows")
    place = lax.axis_index("rows")
    cycles, tile, width = rhs.shape
    panels = inverses.shape[0]
    bf16, f32 = jnp.bfloat16, jnp.float32
    tile_ids = jnp.arange(cycles, dtype=jnp.int32) * count + place

    pairs = [(t, p) for t in range(panels) for p in range(t)]
    blocks = jnp.stack([jnp.where(place == t, factor[0, :, p, :], jnp.zeros((), bf16)) for t, p in pairs])
    blocks = lax.all_gather(lax.psum(blocks, "rows"), "rhs", axis=2, tiled=True)
    block_of = {pair: blocks[i] for i, pair in enumerate(pairs)}

    pivots = lax.all_to_all(rhs[0], "rows", split_axis=1, concat_axis=0, tiled=True)
    sent = []
    for t in range(panels):
        pivot = pivots[t * tile:(t + 1) * tile]
        for p in range(t):
            pivot = pivot - jnp.dot(block_of[t, p], sent[p], preferred_element_type=f32)
        solved = jnp.dot(inverses[t], pivot, precision=lax.Precision.HIGHEST)
        sent.append(solved.astype(bf16))
    every = lax.all_gather(jnp.concatenate(sent, axis=0), "rows", axis=0)
    every = jnp.transpose(every, (1, 0, 2)).reshape(panels * tile, width)

    whole = lax.all_gather(factor, "rhs", axis=3, tiled=True)
    seen = tile_ids[:, None] > jnp.arange(panels, dtype=jnp.int32)[None, :]
    whole = jnp.where(seen[:, None, :, None], whole, jnp.zeros((), bf16))
    whole = whole.reshape(cycles, tile, panels * tile)
    state = rhs - jnp.einsum("crk,kn->crn", whole, every, preferred_element_type=f32)
    at = jnp.minimum(place, panels - 1) * tile
    mine = lax.dynamic_slice_in_dim(every, at, tile, axis=0).astype(f32)
    first = jnp.where(place < panels, mine, state[0])
    return jnp.concatenate([first[None], state[1:]], axis=0)


def solution(mesh):
    return jax.shard_map(
        local,
        mesh=mesh,
        in_specs=(P(None, "rows", "rhs"), P(None, "rows", None, "rhs"), P()),
        out_specs=P(None, "rows", "rhs"),
        check_vma=False,
    )
```
